32 devices in a mesh: member: 4 (over y, x), lat: 2 (over core), lon: 4 (over z).
Axes of the slice: x: 2, y: 2, z: 4, core: 2. Of those that a mesh axis runs over, the one named last changes fastest.
Arguments:
- ice_flux: float32 [8, 64, 8, 512], P(('member', 'lat'), 'lon'), parts along dimension 0, may hold values from 0.5 to 1.5
- ice_frac: float32 [8, 64, 512], P(('member', 'lat'), 'lon'), parts along dimension 0, may hold values from 0.05 to 1
- ice_mask: int32 [8, 64, 512], P(('member', 'lat'), 'lon'), parts along dimension 0, may hold values 0 or 1
- ice_area: float32 [8, 64, 512], P(('member', 'lat'), 'lon'), parts along dimension 0, may hold values from 0.7 to 44.3
- route: int32 [8, 64], P(('member', 'lat'), 'lon'), parts along dimension 0, may hold values from 0 to 63, as said below
- ocean_area: float32 [512, 512], P(('member', 'lat'), 'lon'), parts along dimension 0, may hold values from 0.7 to 44.3
- ocean_wet: int32 [512, 512], P(('member', 'lat'), 'lon'), parts along dimension 0, may hold values 0 or 1
- exponent: int32 [8], replicated, may hold values from 0 to 3
Outputs:
- ocean_flux: float32 [8, 512, 512], P(None, ('member', 'lat'), 'lon'), parts along dimension 1
- source_total: float32 [32], P('member'), parts along dimension 0
The draws below stay inside these ranges and needn't reach their ends.
There are 4 independent parts, one for each index of `member`. The reference program is written for one: setup_inputs(seed, part) draws one part's arguments, and reference() takes and returns one part's arrays. A program takes and returns all parts, laid end to end along the dimension named above; an argument that names none is the same for every part. Nothing has to cross between parts.
Inputs may be any that keep to these rules, and one draw needn't show every extreme that they name: Within each latitude tile row, route is a permutation of 0 to 63. The 16 entries of one device name, for every longitude tile k that they name (route // 16 == k), exactly 4 blocks of it.
All inputs are finite; a program needn't handle non-finite values. No bound on the sum of `ice_mask` or of `ocean_wet` on one device may be relied on, other than what follows from the above.
Results may differ from the reference program's by a relative error of at most 0.0003.
Values sent between devices are 32-bit elements; how exact they have to be, the bound alone decides.
A program may use at most 64 MiB of HBM per device.

```python
import jax
import jax.numpy as jnp

NF = 8
NBT = 16
BLAT = 4
CLON = 128
CLAT = 64
NLATG = 128
NLONG = 512
N_LAT = 2
N_LON = 4


def shuffled(subkey):
    return jax.random.permutation(subkey, jnp.arange(NBT, dtype=jnp.int32))


def offsets_for(subkey):
    return jax.random.permutation(subkey, jnp.arange(N_LON, dtype=jnp.int32))[:NBT // max(2, NBT // N_LON)]


def make_route(key):
    capacity = max(2, NBT // N_LON)
    offset_count = NBT // capacity
    key_offsets, key_slots, key_positions = jax.random.split(jax.random.fold_in(key, 11), 3)
    offsets = jax.vmap(offsets_for)(jax.random.split(key_offsets, N_LAT))
    sequence = jax.vmap(shuffled)(jax.random.split(key_slots, N_LAT * N_LON)).reshape(N_LAT, N_LON, NBT)
    kind_index = sequence // capacity
    offset_table = jnp.broadcast_to(offsets[:, None, :], (N_LAT, N_LON, offset_count))
    chosen = jnp.take_along_axis(offset_table, kind_index, axis=2)
    source_tile = jnp.arange(N_LON, dtype=jnp.int32)[None, :, None]
    target_tile = (source_tile + chosen) % N_LON
    target_positions = jax.vmap(shuffled)(jax.random.split(key_positions, N_LAT * N_LON)).reshape(-1)
    row_number_index = jnp.arange(N_LAT, dtype=jnp.int32)[:, None, None]
    flat_index = (row_number_index * N_LON + target_tile) * NBT + sequence
    block_row = target_positions[flat_index]
    return (target_tile * NBT + block_row).reshape(N_LAT, N_LON * NBT).astype(jnp.int32)


def area_noise(key, shape):
    return jnp.exp(jax.random.uniform(key, shape, jnp.float32, jnp.log(0.7), jnp.log(1.4)))


def profile(lat_cell, lon_cell):
    return jnp.power(10.0, (lat_cell + 0.5) / NLATG) * jnp.power(10.0, 0.5 * (lon_cell + 0.5) / NLONG)


def draw_route(key, part):
    return make_route(key)


def draw_ice_area(key, part):
    route = make_route(key)
    target_tile = route // NBT
    block_row = route % NBT
    within = jnp.arange(BLAT * CLON, dtype=jnp.int32)
    lat_cell = jnp.arange(N_LAT, dtype=jnp.int32)[:, None, None] * CLAT + block_row[:, :, None] * BLAT + (within // CLON)[None, None, :]
    lon_cell = target_tile[:, :, None] * CLON + (within % CLON)[None, None, :]
    reshaped_grid = profile(lat_cell.astype(jnp.float32), lon_cell.astype(jnp.float32))
    return (reshaped_grid * area_noise(jax.random.fold_in(key, 23), reshaped_grid.shape)).astype(jnp.float32)


def draw_ocean_area(key, part):
    lat_cell = jnp.arange(NLATG, dtype=jnp.int32).astype(jnp.float32)[:, None]
    lon_cell = jnp.arange(NLONG, dtype=jnp.int32).astype(jnp.float32)[None, :]
    reshaped_grid = profile(lat_cell, lon_cell)
    return (reshaped_grid * area_noise(jax.random.fold_in(key, 31), reshaped_grid.shape)).astype(jnp.float32)


def touch_ends(entries, rng, low, top_value):
    longest = entries.shape.index(max(entries.shape))
    spots = []
    for shift in (0, 1):
        where = [jax.random.randint(jax.random.fold_in(rng, axis), (), 0, length) for axis, length in enumerate(entries.shape)]
        where[longest] = (where[longest] + shift) % entries.shape[longest]
        spots.append(tuple(where))
    return entries.at[spots[0]].set(low).at[spots[1]].set(top_value)


def steps_of(stream_key, shape, cuts, smallest, top_value):
    loudness, own = 1.0, jax.random.fold_in(stream_key, 6)
    for axis_at, parts in cuts:
        steps = jnp.exp(jax.random.uniform(jax.random.fold_in(own, axis_at), (parts,), jnp.float32, smallest / len(cuts), top_value / len(cuts)))
        loudness = loudness * jnp.repeat(steps, shape[axis_at] // parts).reshape([-1 if axis == axis_at else 1 for axis in range(len(shape))])
    return loudness


def setup_inputs(seed: int = 0, part: int = 0) -> dict:
    splits = jax.random.split(jax.random.key(seed), 9)
    own_keys = jax.random.split(jax.random.fold_in(splits[8], part), 9)
    ice_flux = jnp.clip(0.5 + 1.0 * jax.random.uniform(own_keys[0], (N_LAT, N_LON * NBT, NF, BLAT * CLON), jnp.float32) ** steps_of(own_keys[0], (N_LAT, N_LON * NBT, NF, BLAT * CLON), ((0, 2), (1, 4)), -0.2, 0.2), 0.5, 1.5)
    ice_frac = jnp.clip(0.05 + 0.95 * jax.random.uniform(own_keys[1], (N_LAT, N_LON * NBT, BLAT * CLON), jnp.float32) ** steps_of(own_keys[1], (N_LAT, N_LON * NBT, BLAT * CLON), ((0, 2), (1, 4)), -0.2, 0.2), 0.05, 1.0)
    ice_mask = touch_ends((jax.random.randint(own_keys[2], (N_LAT, N_LON * NBT, BLAT * CLON), 0, 4) < 3).astype(jnp.int32), jax.random.fold_in(own_keys[2], 1), 0, 1)
    ice_area = draw_ice_area(jax.random.fold_in(jax.random.fold_in(splits[8], part), 71), part)
    route = draw_route(jax.random.fold_in(jax.random.fold_in(splits[8], part), 71), part)
    ocean_area = draw_ocean_area(jax.random.fold_in(jax.random.fold_in(splits[8], part), 71), part)
    ocean_wet = touch_ends((jax.random.randint(own_keys[6], (NLATG, NLONG), 0, 4) < 3).astype(jnp.int32), jax.random.fold_in(own_keys[6], 1), 0, 1)
    exponent = touch_ends(jax.random.randint(splits[7], (NF,), 0, 4), jax.random.fold_in(splits[7], 1), 0, 3).astype(jnp.int32)
    return {"ice_flux": ice_flux, "ice_frac": ice_frac, "ice_mask": ice_mask, "ice_area": ice_area, "route": route, "ocean_area": ocean_area, "ocean_wet": ocean_wet, "exponent": exponent}


quantum = 1024.0
limb_base = 65536


def local_units(values, axes):
    return jnp.sum((values * quantum).astype(jnp.int32), axis=axes)


def split_units(total):
    upper_part = total // limb_base
    return upper_part, total - upper_part * limb_base


def join_units(upper_part, lower_part):
    return (upper_part.astype(jnp.float32) * limb_base + lower_part.astype(jnp.float32)) / quantum


def global_integral(units, axes):
    upper_part, lower_part = split_units(units)
    return join_units(jnp.sum(upper_part, axis=axes), jnp.sum(lower_part, axis=axes))


def reference(ice_flux, ice_frac, ice_mask, ice_area, route, ocean_area, ocean_wet, exponent):
    amount = ice_area * ice_frac * ice_mask.astype(jnp.float32)
    carried = ice_flux * amount[:, :, None, :]
    per_device = carried.reshape(N_LAT, N_LON, NBT, NF, BLAT * CLON)
    source = global_integral(local_units(per_device, (2, 4)), (0, 1))
    row_number_index = jnp.broadcast_to(jnp.arange(N_LAT, dtype=jnp.int32)[:, None], route.shape)
    block_groups = jnp.zeros_like(carried).at[row_number_index, route].set(carried)
    mapped = block_groups.reshape(N_LAT, N_LON, NBT, NF, BLAT, CLON).transpose(3, 0, 2, 4, 1, 5).reshape(NF, NLATG, NLONG)
    wet_cover = ocean_wet.astype(jnp.float32)
    wet_cell_terms = (wet_cover * mapped).reshape(NF, N_LAT, CLAT, N_LON, CLON)
    target = global_integral(local_units(wet_cell_terms, (2, 4)), (1, 2))
    area_terms = (ocean_area * wet_cover).reshape(N_LAT, CLAT, N_LON, CLON)
    wet_area = global_integral(local_units(area_terms, (1, 3)), (0, 1))
    correction = (source - target) / wet_area
    scaling = jnp.left_shift(jnp.ones_like(exponent), exponent).astype(jnp.float32)
    ocean_flux = wet_cover * scaling[:, None, None] * (mapped / ocean_area + correction[:, None, None])
    return ocean_flux, source * scaling
```

```python
import functools

import jax
import jax.numpy as jnp
from jax import lax
from jax.experimental import pallas as pl
from jax.experimental.pallas import tpu as pltpu
from jax.sharding import PartitionSpec as P

MESH = pl.DeviceIdType.MESH
quantum = 1024.0
limb_bits = 16
limb_base = 65536.0
lanes = 128


def carry(upper, lower):
    over = jnp.floor(lower * (1.0 / limb_base))
    return upper + over, lower - over * limb_base


def row_limbs(units):
    upper = jnp.sum((units >> limb_bits).astype(jnp.float32), axis=1, keepdims=True)
    lower = jnp.sum((units & 0xFFFF).astype(jnp.float32), axis=1, keepdims=True)
    return carry(upper, lower)


def join(upper, lower):
    return (upper * limb_base + lower) / quantum


def peer_order(count):
    return sorted(range(1, count), key=lambda d: (-min(d, count - d), -d))


def kernel(
    n_lat, n_lon, cap,
    flux_hbm, frac_hbm, mask_hbm, area_hbm, route_hbm, sea_hbm, wet_hbm, exp_hbm,
    out_ref, total_ref,
    flux, frac, mask, area, sea, wet, wetf, inverse, outgoing, received, routes, exps, sums,
    in_sem, route_send, route_recv, bulk_send, bulk_recv, sum_send, sum_recv,
):
    blocks, fields, cells = flux.shape
    rows, width = sea.shape
    band = cells // width
    bits = blocks.bit_length()
    digit = (1 << bits) - 1
    full = cap * n_lon == blocks
    group = n_lat * n_lon
    my_lat = lax.axis_index("lat")
    me = lax.axis_index("lon")

    def peer(offset):
        return {
            "lat": lax.rem(my_lat + offset // n_lon, n_lat),
            "lon": lax.rem(me + offset % n_lon, n_lon),
        }

    loads = [
        pltpu.make_async_copy(src, dst, in_sem.at[i])
        for i, (src, dst) in enumerate((
            (route_hbm, routes.at[pl.ds(0, 1)]), (area_hbm, area), (frac_hbm, frac),
            (mask_hbm, mask), (flux_hbm, flux), (sea_hbm, sea), (wet_hbm, wet), (exp_hbm, exps),
        ))
    ]
    for load in loads:
        load.start()

    barrier = pltpu.get_barrier_semaphore()
    for offset in range(1, group):
        pl.semaphore_signal(barrier, inc=1, device_id=peer(offset), device_id_type=MESH)

    loads[0].wait()

    def digits_of(slot, low, value):
        packed = jnp.int32(0)
        for s in range(blocks):
            r = routes[slot, s]
            hit = (r >= low) & (r < low + blocks)
            packed = jnp.where(hit, (packed << bits) + (value(s, r - low) + 1), packed)
        return [(packed >> (bits * (cap - 1 - c))) & digit for c in range(cap)]

    chosen = {}
    order = peer_order(n_lon) + [0]
    for d in order:
        low = lax.rem(me + d, n_lon) * blocks
        chosen[d] = [jnp.maximum(v - 1, 0) for v in digits_of(0, low, lambda s, row: s)]

    for load in loads[1:5]:
        load.wait()
    pl.semaphore_wait(barrier, group - 1)

    route_copies = {}
    for d in order[:-1]:
        route_copies[d] = pltpu.make_async_remote_copy(
            src_ref=route_hbm, dst_ref=routes.at[pl.ds(d, 1)],
            send_sem=route_send.at[d - 1], recv_sem=route_recv.at[d - 1],
            device_id=peer(d), device_id_type=MESH,
        )
        route_copies[d].start()

    bulk = {}
    for d in order:
        for c in range(cap):
            s = chosen[d][c]
            here = pl.ds(s, 1)
            amount = area[here, :] * frac[here, :] * mask[here, :].astype(jnp.float32)
            block = flux[s] * amount
            if d:
                outgoing[(d - 1) * cap + c] = block
            else:
                received[c] = block
        if d:
            bulk[d] = pltpu.make_async_remote_copy(
                src_ref=outgoing.at[pl.ds((d - 1) * cap, cap)],
                dst_ref=received.at[pl.ds(d * cap, cap)],
                send_sem=bulk_send.at[d - 1], recv_sem=bulk_recv.at[d - 1],
                device_id=peer(d), device_id_type=MESH,
            )
            bulk[d].start()

    source_units = jnp.zeros((fields, width), jnp.int32)
    for s in range(blocks):
        here = pl.ds(s, 1)
        amount = area[here, :] * frac[here, :] * mask[here, :].astype(jnp.float32)
        units = (flux[s] * amount * quantum).astype(jnp.int32)
        for r in range(band):
            source_units += units[:, r * width : (r + 1) * width]

    for load in loads[5:]:
        load.wait()
    wetf[...] = wet[...].astype(jnp.float32)
    inverse[...] = wetf[...] / sea[...]
    area_units = jnp.zeros((8, width), jnp.int32)
    for i in range(rows // 8):
        part = pl.ds(i * 8, 8)
        area_units += (sea[part, :] * wetf[part, :] * quantum).astype(jnp.int32)

    sub = lax.broadcasted_iota(jnp.int32, (8, lanes), 0)
    lane = lax.broadcasted_iota(jnp.int32, (8, lanes), 1)

    def placed(values, first):
        return sum(
            jnp.where(lane == sub + (first + i) * 8, v, 0.0) for i, v in enumerate(values)
        )

    early = placed(row_limbs(source_units) + row_limbs(area_units), 0)
    power = jnp.zeros((8, lanes), jnp.int32)
    power_row = jnp.zeros((1, lanes), jnp.int32)
    for f in range(fields):
        power = jnp.where(sub == f, exps[f], power)
        power_row = jnp.where(lane[:1] == f, exps[f], power_row)
    scaling = jnp.left_shift(jnp.ones_like(power), power).astype(jnp.float32)
    scaling_row = jnp.left_shift(jnp.ones_like(power_row), power_row).astype(jnp.float32)

    low = me * blocks
    slot_of = [jnp.int32(0)] * blocks
    target_units = jnp.zeros((fields, width), jnp.int32)
    for d in [0] + order[:-1]:
        if d:
            route_copies[d].wait_recv()
        digits = digits_of(d, low, lambda s, row: row)
        for c in range(cap):
            for n in range(blocks):
                slot_of[n] = jnp.where(digits[c] == n + 1, d * cap + c, slot_of[n])
        if d:
            bulk[d].wait_recv()
        for c in range(cap):
            row = jnp.maximum(digits[c] - 1, 0)
            for r in range(band):
                cover = wetf[pl.ds(row * band + r, 1), :]
                value = received[d * cap + c, :, r * width : (r + 1) * width]
                units = (cover * value * quantum).astype(jnp.int32)
                if not full:
                    units = units * jnp.minimum(digits[c], 1)
                target_units += units

    mine = jnp.sum(early + placed(row_limbs(target_units), 4), axis=0, keepdims=True)
    sums[pl.ds(0, 1), :] = mine
    sum_copies = []
    for offset in range(1, group):
        copy = pltpu.make_async_remote_copy(
            src_ref=sums.at[pl.ds(0, 1)], dst_ref=sums.at[pl.ds(offset, 1)],
            send_sem=sum_send.at[offset - 1], recv_sem=sum_recv.at[offset - 1],
            device_id=peer(offset), device_id_type=MESH,
        )
        copy.start()
        sum_copies.append(copy)
    for copy in sum_copies:
        copy.wait_recv()

    whole = jnp.sum(sums[...], axis=0, keepdims=True)

    def taken(i):
        return jnp.sum(jnp.where(lane == sub + i * 8, whole, 0.0), axis=1, keepdims=True)

    source = join(taken(0), taken(1))
    wet_upper, wet_lower = carry(taken(2), taken(3))
    wet_area = join(
        jnp.sum(wet_upper, axis=0, keepdims=True), jnp.sum(wet_lower, axis=0, keepdims=True)
    )
    target = join(taken(4), taken(5))
    offset_value = scaling * ((source - target) / wet_area)

    for n in range(blocks):
        slot = slot_of[n]
        for r in range(band):
            line = n * band + r
            value = received[slot, :, r * width : (r + 1) * width]
            result = scaling * (value * inverse[line : line + 1, :])
            result = result + offset_value * wetf[line : line + 1, :]
            out_ref[pl.ds(line, fields, stride=rows), :] = result

    aligned = pltpu.roll(whole, lanes - 8, 1)
    total_ref[...] = join(whole, aligned) * scaling_row

    for copy in sum_copies:
        copy.wait_send()
    for d in order[:-1]:
        route_copies[d].wait_send()
        bulk[d].wait_send()


def solution(mesh):
    n_lat, n_lon = mesh.shape["lat"], mesh.shape["lon"]

    def body(ice_flux, ice_frac, ice_mask, ice_area, route, ocean_area, ocean_wet, exponent):
        blocks, fields, cells = ice_flux.shape[1:]
        rows, width = ocean_area.shape
        cap = max(2, blocks // n_lon)
        group = n_lat * n_lon
        anywhere = pl.BlockSpec(memory_space=pl.ANY)
        vmem = pl.BlockSpec(memory_space=pltpu.VMEM)
        dma = pltpu.SemaphoreType.DMA
        flux_out, total = pl.pallas_call(
            functools.partial(kernel, n_lat, n_lon, cap),
            out_shape=(
                jax.ShapeDtypeStruct((fields * rows, width), jnp.float32),
                jax.ShapeDtypeStruct((1, lanes), jnp.float32),
            ),
            in_specs=[anywhere] * 8,
            out_specs=(vmem, vmem),
            scratch_shapes=[
                pltpu.VMEM((blocks, fields, cells), jnp.float32),
                pltpu.VMEM((blocks, cells), jnp.float32),
                pltpu.VMEM((blocks, cells), jnp.int32),
                pltpu.VMEM((blocks, cells), jnp.float32),
                pltpu.VMEM((rows, width), jnp.float32),
                pltpu.VMEM((rows, width), jnp.int32),
                pltpu.VMEM((rows, width), jnp.float32),
                pltpu.VMEM((rows, width), jnp.float32),
                pltpu.VMEM(((n_lon - 1) * cap, fields, cells), jnp.float32),
                pltpu.VMEM((n_lon * cap, fields, cells), jnp.float32),
                pltpu.SMEM((n_lon, blocks), jnp.int32),
                pltpu.SMEM((fields,), jnp.int32),
                pltpu.VMEM((group, lanes), jnp.float32),
                dma((8,)),
                dma((n_lon - 1,)), dma((n_lon - 1,)),
                dma((n_lon - 1,)), dma((n_lon - 1,)),
                dma((group - 1,)), dma((group - 1,)),
            ],
            compiler_params=pltpu.CompilerParams(collective_id=0, has_side_effects=True),
        )(
            ice_flux[0], ice_frac[0], ice_mask[0], ice_area[0],
            route, ocean_area, ocean_wet, exponent,
        )
        return flux_out.reshape(fields, rows, width), total[0, :fields]

    placed = (
        P(("member", "lat"), "lon", None, None),
        P(("member", "lat"), "lon", None),
        P(("member", "lat"), "lon", None),
        P(("member", "lat"), "lon", None),
        P(("member", "lat"), "lon"),
        P(("member", "lat"), "lon"),
        P(("member", "lat"), "lon"),
        P(),
    )
    return jax.shard_map(
        body,
        mesh=mesh,
        in_specs=placed,
        out_specs=(P(None, ("member", "lat"), "lon"), P("member")),
        check_vma=False,
    )
```

```python
import functools

import jax
import jax.numpy as jnp
from jax import lax
from jax.experimental import pallas as pl
from jax.experimental.pallas import tpu as pltpu
from jax.sharding import PartitionSpec as P

MESH = pl.DeviceIdType.MESH
quantum = 1024.0
limb_bits = 16
limb_base = 65536.0
lanes = 128


def carry(upper, lower):
    over = jnp.floor(lower * (1.0 / limb_base))
    return upper + over, lower - over * limb_base


def row_limbs(units):
    upper = jnp.sum((units >> limb_bits).astype(jnp.float32), axis=1, keepdims=True)
    lower = jnp.sum((units & 0xFFFF).astype(jnp.float32), axis=1, keepdims=True)
    return carry(upper, lower)


def join(upper, lower):
    return (upper * limb_base + lower) / quantum


def send_steps(count):
    table = []
    for me in range(count):
        near = sorted((p for p in range(count) if p != me), key=lambda p: (abs(p - me), p))
        table.append(near[-1:] + near[:-1])
    return [[row[step] for row in table] for step in range(count - 1)]


def kernel(
    n_lat, n_lon, cap,
    flux_hbm, frac_hbm, mask_hbm, area_hbm, route_hbm, sea_hbm, wet_hbm, exp_hbm,
    ordered, wetf, coefs, total_ref,
    flux, frac, mask, area, sea, wet, inverse, outgoing, received, routes, exps, sums,
    in_sem, route_send, route_recv, bulk_send, bulk_recv, sum_send, sum_recv,
):
    blocks, fields, cells = flux.shape
    rows, width = sea.shape
    band = cells // width
    bits = blocks.bit_length()
    digit = (1 << bits) - 1
    full = cap * n_lon == blocks
    group = n_lat * n_lon
    my_lat = lax.axis_index("lat")
    me = lax.axis_index("lon")

    def peer(offset):
        return {
            "lat": lax.rem(my_lat + offset // n_lon, n_lat),
            "lon": lax.rem(me + offset % n_lon, n_lon),
        }

    loads = [
        pltpu.make_async_copy(src, dst, in_sem.at[i])
        for i, (src, dst) in enumerate((
            (route_hbm, routes.at[pl.ds(0, 1)]), (area_hbm, area), (frac_hbm, frac),
            (mask_hbm, mask), (flux_hbm, flux), (sea_hbm, sea), (wet_hbm, wet), (exp_hbm, exps),
        ))
    ]
    for load in loads:
        load.start()

    barrier = pltpu.get_barrier_semaphore()
    for offset in range(1, group):
        pl.semaphore_signal(barrier, inc=1, device_id=peer(offset), device_id_type=MESH)

    loads[0].wait()

    def digits_of(slot, low, value):
        packed = jnp.int32(0)
        for s in range(blocks):
            r = routes[slot, s]
            hit = (r >= low) & (r < low + blocks)
            packed = jnp.where(hit, (packed << bits) + (value(s, r - low) + 1), packed)
        return [(packed >> (bits * (cap - 1 - c))) & digit for c in range(cap)]

    pl.semaphore_wait(barrier, group - 1)

    if n_lon ** n_lon < 2 ** 31:
        place = 1
        for i in range(n_lon - 1):
            place = place * (1 + (n_lon - 1) * ((me + n_lon - 1 - i) // n_lon))
        steps = [
            sum(t * n_lon ** i for i, t in enumerate(row)) // place % n_lon
            for row in send_steps(n_lon)
        ]
    else:
        steps = [lax.rem(me + d, n_lon) for d in range(1, n_lon)]
    away = [lax.rem(target - me + n_lon, n_lon) for target in steps]

    def lon_copy(src, dst, send, recv, d, target):
        return pltpu.make_async_remote_copy(
            src_ref=src, dst_ref=dst, send_sem=send.at[d - 1], recv_sem=recv.at[d - 1],
            device_id={"lat": my_lat, "lon": target}, device_id_type=MESH,
        )

    route_copies = [
        lon_copy(routes.at[pl.ds(0, 1)], routes.at[pl.ds(d, 1)], route_send, route_recv, d, t)
        for d, t in zip(away, steps)
    ]
    for copy in route_copies:
        copy.start()

    chosen = [
        [jnp.maximum(v - 1, 0) for v in digits_of(0, target * blocks, lambda s, row: s)]
        for target in steps + [me]
    ]
    for load in loads[1:5]:
        load.wait()

    bulk = []
    for step, picks in enumerate(chosen):
        last = step == n_lon - 1
        for c, s in enumerate(picks):
            here = pl.ds(s, 1)
            amount = area[here, :] * frac[here, :] * mask[here, :].astype(jnp.float32)
            block = flux[s] * amount
            if last:
                received[c] = block
            else:
                outgoing[step * cap + c] = block
        if not last:
            d = away[step]
            bulk.append(lon_copy(
                outgoing.at[pl.ds(step * cap, cap)], received.at[pl.ds(d * cap, cap)],
                bulk_send, bulk_recv, d, steps[step],
            ))
            bulk[-1].start()

    def arrival(d):
        here = received.at[pl.ds(d * cap, cap)]
        line = routes.at[pl.ds(d, 1)]
        source = lax.rem(me - d + n_lon, n_lon)
        return (
            lon_copy(line, line, route_send, route_recv, d, source),
            lon_copy(here, here, bulk_send, bulk_recv, d, source),
        )

    source_units = jnp.zeros((fields, width), jnp.int32)
    for s in range(blocks):
        here = pl.ds(s, 1)
        amount = area[here, :] * frac[here, :] * mask[here, :].astype(jnp.float32)
        units = (flux[s] * amount * quantum).astype(jnp.int32)
        for r in range(band):
            source_units += units[:, r * width : (r + 1) * width]

    for load in loads[5:]:
        load.wait()
    wetf[...] = wet[...].astype(jnp.float32)
    inverse[...] = wetf[...] / sea[...]
    area_units = jnp.zeros((8, width), jnp.int32)
    for i in range(rows // 8):
        part = pl.ds(i * 8, 8)
        area_units += (sea[part, :] * wetf[part, :] * quantum).astype(jnp.int32)

    sub = lax.broadcasted_iota(jnp.int32, (8, lanes), 0)
    lane = lax.broadcasted_iota(jnp.int32, (8, lanes), 1)

    def placed(values, first):
        return sum(
            jnp.where(lane == sub + (first + i) * 8, v, 0.0) for i, v in enumerate(values)
        )

    early = placed(row_limbs(source_units) + row_limbs(area_units), 0)
    power = jnp.zeros((8, lanes), jnp.int32)
    power_row = jnp.zeros((1, lanes), jnp.int32)
    for f in range(fields):
        power = jnp.where(sub == f, exps[f], power)
        power_row = jnp.where(lane[:1] == f, exps[f], power_row)
    scaling = jnp.left_shift(jnp.ones_like(power), power).astype(jnp.float32)
    scaling_row = jnp.left_shift(jnp.ones_like(power_row), power_row).astype(jnp.float32)

    low = me * blocks
    slot_of = [jnp.int32(0)] * blocks
    target_units = jnp.zeros((fields, width), jnp.int32)
    near_first = sorted(range(n_lon), key=lambda d: min(d, n_lon - d))
    for d in near_first:
        if d:
            route_arrival, bulk_arrival = arrival(d)
            route_arrival.wait_recv()
        digits = digits_of(d, low, lambda s, row: row)
        for c in range(cap):
            for n in range(blocks):
                slot_of[n] = jnp.where(digits[c] == n + 1, d * cap + c, slot_of[n])
        if d:
            bulk_arrival.wait_recv()
        for c in range(cap):
            row = jnp.maximum(digits[c] - 1, 0)
            for r in range(band):
                cover = wetf[pl.ds(row * band + r, 1), :]
                value = received[d * cap + c, :, r * width : (r + 1) * width]
                units = (cover * value * quantum).astype(jnp.int32)
                if not full:
                    units = units * jnp.minimum(digits[c], 1)
                target_units += units

    mine = jnp.sum(early + placed(row_limbs(target_units), 4), axis=0, keepdims=True)
    sums[pl.ds(0, 1), :] = mine
    sum_copies = []
    for offset in range(1, group):
        copy = pltpu.make_async_remote_copy(
            src_ref=sums.at[pl.ds(0, 1)], dst_ref=sums.at[pl.ds(offset, 1)],
            send_sem=sum_send.at[offset - 1], recv_sem=sum_recv.at[offset - 1],
            device_id=peer(offset), device_id_type=MESH,
        )
        copy.start()
        sum_copies.append(copy)
    for n in range(blocks):
        slot = slot_of[n]
        for r in range(band):
            line = n * band + r
            value = received[slot, :, r * width : (r + 1) * width]
            ordered[pl.ds(line, fields, stride=rows), :] = value * inverse[line : line + 1, :]

    for copy in sum_copies:
        copy.wait_recv()

    whole = jnp.sum(sums[...], axis=0, keepdims=True)

    def taken(i):
        return jnp.sum(jnp.where(lane == sub + i * 8, whole, 0.0), axis=1, keepdims=True)

    source = join(taken(0), taken(1))
    wet_upper, wet_lower = carry(taken(2), taken(3))
    wet_area = join(
        jnp.sum(wet_upper, axis=0, keepdims=True), jnp.sum(wet_lower, axis=0, keepdims=True)
    )
    target = join(taken(4), taken(5))
    coefs[0] = scaling
    coefs[1] = scaling * ((source - target) / wet_area)

    aligned = pltpu.roll(whole, lanes - 8, 1)
    total_ref[...] = join(whole, aligned) * scaling_row

    for copy in sum_copies + route_copies + bulk:
        copy.wait_send()


def finish(ordered, wetf, coefs, total_row, out_hbm, total_ref, out, sems):
    fields = total_ref.shape[0]
    rows = wetf.shape[0]
    copies = []
    for f in range(fields):
        here = pl.ds(f * rows, rows)
        out[here, :] = ordered[here, :] * coefs[0, f : f + 1, :] + wetf[...] * coefs[1, f : f + 1, :]
        copies.append(pltpu.make_async_copy(out.at[here], out_hbm.at[here], sems.at[f]))
        copies[-1].start()
    total_ref[...] = total_row[0, :fields]
    for copy in copies:
        copy.wait()


def solution(mesh):
    n_lat, n_lon = mesh.shape["lat"], mesh.shape["lon"]

    def body(ice_flux, ice_frac, ice_mask, ice_area, route, ocean_area, ocean_wet, exponent):
        blocks, fields, cells = ice_flux.shape[1:]
        rows, width = ocean_area.shape
        cap = max(2, blocks // n_lon)
        group = n_lat * n_lon
        anywhere = pl.BlockSpec(memory_space=pl.ANY)
        vmem = pl.BlockSpec(memory_space=pltpu.VMEM)
        dma = pltpu.SemaphoreType.DMA
        near = pl.pallas_call(
            functools.partial(kernel, n_lat, n_lon, cap),
            out_shape=(
                pltpu.VMEM((fields * rows, width), jnp.float32),
                pltpu.VMEM((rows, width), jnp.float32),
                pltpu.VMEM((2, fields, lanes), jnp.float32),
                pltpu.VMEM((1, lanes), jnp.float32),
            ),
            in_specs=[anywhere] * 8,
            out_specs=(vmem,) * 4,
            scratch_shapes=[
                pltpu.VMEM((blocks, fields, cells), jnp.float32),
                pltpu.VMEM((blocks, cells), jnp.float32),
                pltpu.VMEM((blocks, cells), jnp.int32),
                pltpu.VMEM((blocks, cells), jnp.float32),
                pltpu.VMEM((rows, width), jnp.float32),
                pltpu.VMEM((rows, width), jnp.int32),
                pltpu.VMEM((rows, width), jnp.float32),
                pltpu.VMEM(((n_lon - 1) * cap, fields, cells), jnp.float32),
                pltpu.VMEM((n_lon * cap, fields, cells), jnp.float32),
                pltpu.SMEM((n_lon, blocks), jnp.int32),
                pltpu.SMEM((fields,), jnp.int32),
                pltpu.VMEM((group, lanes), jnp.float32),
                dma((8,)),
                dma((n_lon - 1,)), dma((n_lon - 1,)),
                dma((n_lon - 1,)), dma((n_lon - 1,)),
                dma((group - 1,)), dma((group - 1,)),
            ],
            compiler_params=pltpu.CompilerParams(collective_id=0, has_side_effects=True),
        )(
            ice_flux[0], ice_frac[0], ice_mask[0], ice_area[0],
            route, ocean_area, ocean_wet, exponent,
        )
        flux_out, total = pl.pallas_call(
            finish,
            out_shape=(
                jax.ShapeDtypeStruct((fields * rows, width), jnp.float32),
                jax.ShapeDtypeStruct((fields,), jnp.float32),
            ),
            in_specs=[vmem] * 4,
            out_specs=(anywhere, vmem),
            scratch_shapes=[pltpu.VMEM((fields * rows, width), jnp.float32), dma((fields,))],
        )(*(pltpu.with_memory_space_constraint(x, pltpu.VMEM) for x in near))
        return flux_out.reshape(fields, rows, width), total

    placed = (
        P(("member", "lat"), "lon", None, None),
        P(("member", "lat"), "lon", None),
        P(("member", "lat"), "lon", None),
        P(("member", "lat"), "lon", None),
        P(("member", "lat"), "lon"),
        P(("member", "lat"), "lon"),
        P(("member", "lat"), "lon"),
        P(),
    )
    return jax.shard_map(
        body,
        mesh=mesh,
        in_specs=placed,
        out_specs=(P(None, ("member", "lat"), "lon"), P("member")),
        check_vma=False,
    )
```

```python
import functools

import jax
import jax.numpy as jnp
from jax import lax
from jax.experimental import pallas as pl
from jax.experimental.pallas import tpu as pltpu
from jax.sharding import PartitionSpec as P

MESH = pl.DeviceIdType.MESH
quantum = 1024.0
limb_bits = 16
limb_base = 65536.0
lanes = 128


def carry(upper, lower):
    over = jnp.floor(lower * (1.0 / limb_base))
    return upper + over, lower - over * limb_base


def row_limbs(units):
    upper = jnp.sum((units >> limb_bits).astype(jnp.float32), axis=1, keepdims=True)
    lower = jnp.sum((units & 0xFFFF).astype(jnp.float32), axis=1, keepdims=True)
    return carry(upper, lower)


def join(upper, lower):
    return (upper * limb_base + lower) / quantum


def plan(count):
    middle = (count - 1) / 2
    sends = []
    for me in range(count):
        near = sorted(
            (p for p in range(count) if p != me),
            key=lambda p: (abs(p - me), -((p - me) * (middle - me) > 0)),
        )
        sends.append(near[-1:] + near[:-1])
    late = [row[-1] for row in sends]
    if count ** count >= 2 ** 31 or sorted(late) != list(range(count)):
        return None
    sources = []
    for me in range(count):
        last = late.index(me)
        early = sorted(
            (p for p in range(count) if p not in (me, last)), key=lambda p: abs(p - me)
        )
        sources.append(early + [last])
    return sends, sources


def kernel(
    n_lat, n_lon, cap,
    flux_hbm, frac_hbm, mask_hbm, area_hbm, route_hbm, sea_hbm, wet_hbm, exp_hbm,
    ordered, wetf, coefs, total_ref,
    flux, frac, mask, area, sea, wet, inverse, outgoing, received, routes, exps, sums, cover_out, cover_in,
    in_sem, route_send, route_recv, bulk_send, bulk_recv, sum_send, sum_recv, cover_sem,
):
    blocks, fields, cells = flux.shape
    rows, width = sea.shape
    band = cells // width
    bits = blocks.bit_length()
    digit = (1 << bits) - 1
    full = cap * n_lon == blocks
    group = n_lat * n_lon
    my_lat = lax.axis_index("lat")
    me = lax.axis_index("lon")

    def peer(offset):
        return {
            "lat": lax.rem(my_lat + offset // n_lon, n_lat),
            "lon": lax.rem(me + offset % n_lon, n_lon),
        }

    loads = [
        pltpu.make_async_copy(src, dst, in_sem.at[i])
        for i, (src, dst) in enumerate((
            (route_hbm, routes.at[pl.ds(0, 1)]), (area_hbm, area), (frac_hbm, frac),
            (mask_hbm, mask), (flux_hbm, flux), (sea_hbm, sea), (wet_hbm, wet), (exp_hbm, exps),
        ))
    ]
    for load in loads:
        load.start()

    barrier = pltpu.get_barrier_semaphore()
    for offset in range(1, group):
        pl.semaphore_signal(barrier, inc=1, device_id=peer(offset), device_id_type=MESH)

    loads[0].wait()

    def digits_of(slot, low, value):
        packed = jnp.int32(0)
        for s in range(blocks):
            r = routes[slot, s]
            hit = (r >= low) & (r < low + blocks)
            packed = jnp.where(hit, (packed << bits) + (value(s, r - low) + 1), packed)
        return [(packed >> (bits * (cap - 1 - c))) & digit for c in range(cap)]

    planned = plan(n_lon)
    if planned:
        place = 1
        for i in range(n_lon - 1):
            place = place * (1 + (n_lon - 1) * ((me + n_lon - 1 - i) // n_lon))
        steps, sources = (
            [
                sum(row[step] * n_lon ** i for i, row in enumerate(table)) // place % n_lon
                for step in range(n_lon - 1)
            ]
            for table in planned
        )
    else:
        steps = [lax.rem(me + d, n_lon) for d in range(1, n_lon)]
        sources = [lax.rem(me + n_lon - d, n_lon) for d in range(1, n_lon)]
    away = [lax.rem(target - me + n_lon, n_lon) for target in steps]
    behind = [lax.rem(me - source + n_lon, n_lon) for source in sources]

    def lon_copy(src, dst, send, recv, target):
        return pltpu.make_async_remote_copy(
            src_ref=src, dst_ref=dst, send_sem=send, recv_sem=recv,
            device_id={"lat": my_lat, "lon": target}, device_id_type=MESH,
        )

    def route_copy(d, src, target):
        return lon_copy(
            routes.at[pl.ds(src, 1)], routes.at[pl.ds(d, 1)],
            route_send.at[d - 1], route_recv.at[d - 1], target,
        )

    def bulk_copy(d, src, first, target):
        return lon_copy(
            src.at[pl.ds(first, cap)], received.at[pl.ds(d * cap, cap)],
            bulk_send.at[d - 1], bulk_recv.at[d - 1], target,
        )

    def fill(target, dst, first):
        picks = digits_of(0, target * blocks, lambda s, row: s)
        for c, pick in enumerate(picks):
            s = jnp.maximum(pick - 1, 0)
            here = pl.ds(s, 1)
            amount = area[here, :] * frac[here, :] * mask[here, :].astype(jnp.float32)
            dst[first + c] = flux[s] * amount

    for load in loads[1:5]:
        load.wait()
    for step, target in enumerate(steps):
        fill(target, outgoing, step * cap)

    pl.semaphore_wait(barrier, group - 1)
    route_copies = [route_copy(d, 0, target) for d, target in zip(away, steps)]
    bulk = [
        bulk_copy(d, outgoing, step * cap, target)
        for step, (d, target) in enumerate(zip(away, steps))
    ]
    for copy in route_copies + bulk[:1]:
        copy.start()
    fill(me, received, 0)

    for load in loads[5:]:
        load.wait()
    wetf[...] = wet[...].astype(jnp.float32)

    low = me * blocks
    last_source, last_behind = sources[-1], behind[-1]
    route_copy(last_behind, last_behind, last_source).wait_recv()
    last_digits = digits_of(last_behind, low, lambda s, row: row)
    for c, pick in enumerate(last_digits):
        row = jnp.maximum(pick - 1, 0)
        for r in range(band):
            cover = wetf[pl.ds(row * band + r, 1), :]
            if not full:
                cover = cover * jnp.minimum(pick, 1).astype(jnp.float32)
            cover_out[pl.ds(c * band + r, 1), :] = cover
    cover_copy = lon_copy(cover_out, cover_in, cover_sem.at[0], cover_sem.at[1], last_source)
    cover_copy.start()
    for copy in bulk[1:]:
        copy.start()

    source_units = jnp.zeros((fields, width), jnp.int32)
    for s in range(blocks):
        here = pl.ds(s, 1)
        amount = area[here, :] * frac[here, :] * mask[here, :].astype(jnp.float32)
        units = (flux[s] * amount * quantum).astype(jnp.int32)
        for r in range(band):
            source_units += units[:, r * width : (r + 1) * width]

    inverse[...] = wetf[...] / sea[...]
    area_units = jnp.zeros((8, width), jnp.int32)
    for i in range(rows // 8):
        part = pl.ds(i * 8, 8)
        area_units += (sea[part, :] * wetf[part, :] * quantum).astype(jnp.int32)

    sub = lax.broadcasted_iota(jnp.int32, (8, lanes), 0)
    lane = lax.broadcasted_iota(jnp.int32, (8, lanes), 1)

    def placed(values, first):
        return sum(
            jnp.where(lane == sub + (first + i) * 8, v, 0.0) for i, v in enumerate(values)
        )

    early = placed(row_limbs(source_units) + row_limbs(area_units), 0)
    power = jnp.zeros((8, lanes), jnp.int32)
    power_row = jnp.zeros((1, lanes), jnp.int32)
    for f in range(fields):
        power = jnp.where(sub == f, exps[f], power)
        power_row = jnp.where(lane[:1] == f, exps[f], power_row)
    scaling = jnp.left_shift(jnp.ones_like(power), power).astype(jnp.float32)
    scaling_row = jnp.left_shift(jnp.ones_like(power_row), power_row).astype(jnp.float32)

    slot_of = [jnp.int32(0)] * blocks

    def settle(d, digits):
        for c in range(cap):
            for n in range(blocks):
                slot_of[n] = jnp.where(digits[c] == n + 1, d * cap + c, slot_of[n])

    settle(last_behind, last_digits)
    target_units = jnp.zeros((fields, width), jnp.int32)
    for d, source in [(0, me)] + list(zip(behind, sources))[:-1]:
        if source is not me:
            route_copy(d, d, source).wait_recv()
        digits = digits_of(d, low, lambda s, row: row)
        settle(d, digits)
        if source is not me:
            bulk_copy(d, received, d * cap, source).wait_recv()
        for c in range(cap):
            row = jnp.maximum(digits[c] - 1, 0)
            for r in range(band):
                cover = wetf[pl.ds(row * band + r, 1), :]
                value = received[d * cap + c, :, r * width : (r + 1) * width]
                units = (cover * value * quantum).astype(jnp.int32)
                if not full:
                    units = units * jnp.minimum(digits[c], 1)
                target_units += units

    cover_copy.wait_recv()
    for c in range(cap):
        for r in range(band):
            cover = cover_in[c * band + r : c * band + r + 1, :]
            value = outgoing[(n_lon - 2) * cap + c, :, r * width : (r + 1) * width]
            target_units += (cover * value * quantum).astype(jnp.int32)

    mine = jnp.sum(early + placed(row_limbs(target_units), 4), axis=0, keepdims=True)
    sums[pl.ds(0, 1), :] = mine
    sum_copies = []
    for offset in range(1, group):
        copy = pltpu.make_async_remote_copy(
            src_ref=sums.at[pl.ds(0, 1)], dst_ref=sums.at[pl.ds(offset, 1)],
            send_sem=sum_send.at[offset - 1], recv_sem=sum_recv.at[offset - 1],
            device_id=peer(offset), device_id_type=MESH,
        )
        copy.start()
        sum_copies.append(copy)
    bulk_copy(last_behind, received, last_behind * cap, last_source).wait_recv()
    for n in range(blocks):
        slot = slot_of[n]
        for r in range(band):
            line = n * band + r
            value = received[slot, :, r * width : (r + 1) * width]
            ordered[pl.ds(line, fields, stride=rows), :] = value * inverse[line : line + 1, :]

    for copy in sum_copies:
        copy.wait_recv()

    whole = jnp.sum(sums[...], axis=0, keepdims=True)

    def taken(i):
        return jnp.sum(jnp.where(lane == sub + i * 8, whole, 0.0), axis=1, keepdims=True)

    source = join(taken(0), taken(1))
    wet_upper, wet_lower = carry(taken(2), taken(3))
    wet_area = join(
        jnp.sum(wet_upper, axis=0, keepdims=True), jnp.sum(wet_lower, axis=0, keepdims=True)
    )
    target = join(taken(4), taken(5))
    coefs[0] = scaling
    coefs[1] = scaling * ((source - target) / wet_area)

    aligned = pltpu.roll(whole, lanes - 8, 1)
    total_ref[...] = join(whole, aligned) * scaling_row

    for copy in sum_copies + route_copies + bulk + [cover_copy]:
        copy.wait_send()


def finish(ordered, wetf, coefs, total_row, out_hbm, total_ref, out, sems):
    fields = total_ref.shape[0]
    rows = wetf.shape[0]
    copies = []
    for f in range(fields):
        here = pl.ds(f * rows, rows)
        out[here, :] = ordered[here, :] * coefs[0, f : f + 1, :] + wetf[...] * coefs[1, f : f + 1, :]
        copies.append(pltpu.make_async_copy(out.at[here], out_hbm.at[here], sems.at[f]))
        copies[-1].start()
    total_ref[...] = total_row[0, :fields]
    for copy in copies:
        copy.wait()


def solution(mesh):
    n_lat, n_lon = mesh.shape["lat"], mesh.shape["lon"]

    def body(ice_flux, ice_frac, ice_mask, ice_area, route, ocean_area, ocean_wet, exponent):
        blocks, fields, cells = ice_flux.shape[1:]
        rows, width = ocean_area.shape
        cap = max(2, blocks // n_lon)
        group = n_lat * n_lon
        anywhere = pl.BlockSpec(memory_space=pl.ANY)
        vmem = pl.BlockSpec(memory_space=pltpu.VMEM)
        dma = pltpu.SemaphoreType.DMA
        near = pl.pallas_call(
            functools.partial(kernel, n_lat, n_lon, cap),
            out_shape=(
                pltpu.VMEM((fields * rows, width), jnp.float32),
                pltpu.VMEM((rows, width), jnp.float32),
                pltpu.VMEM((2, fields, lanes), jnp.float32),
                pltpu.VMEM((1, lanes), jnp.float32),
            ),
            in_specs=[anywhere] * 8,
            out_specs=(vmem,) * 4,
            scratch_shapes=[
                pltpu.VMEM((blocks, fields, cells), jnp.float32),
                pltpu.VMEM((blocks, cells), jnp.float32),
                pltpu.VMEM((blocks, cells), jnp.int32),
                pltpu.VMEM((blocks, cells), jnp.float32),
                pltpu.VMEM((rows, width), jnp.float32),
                pltpu.VMEM((rows, width), jnp.int32),
                pltpu.VMEM((rows, width), jnp.float32),
                pltpu.VMEM(((n_lon - 1) * cap, fields, cells), jnp.float32),
                pltpu.VMEM((n_lon * cap, fields, cells), jnp.float32),
                pltpu.SMEM((n_lon, blocks), jnp.int32),
                pltpu.SMEM((fields,), jnp.int32),
                pltpu.VMEM((group, lanes), jnp.float32),
                pltpu.VMEM((cap * cells // width, width), jnp.float32),
                pltpu.VMEM((cap * cells // width, width), jnp.float32),
                dma((8,)),
                dma((n_lon - 1,)), dma((n_lon - 1,)),
                dma((n_lon - 1,)), dma((n_lon - 1,)),
                dma((group - 1,)), dma((group - 1,)), dma((2,)),
            ],
            compiler_params=pltpu.CompilerParams(collective_id=0, has_side_effects=True),
        )(
            ice_flux[0], ice_frac[0], ice_mask[0], ice_area[0],
            route, ocean_area, ocean_wet, exponent,
        )
        flux_out, total = pl.pallas_call(
            finish,
            out_shape=(
                jax.ShapeDtypeStruct((fields * rows, width), jnp.float32),
                jax.ShapeDtypeStruct((fields,), jnp.float32),
            ),
            in_specs=[vmem] * 4,
            out_specs=(anywhere, vmem),
            scratch_shapes=[pltpu.VMEM((fields * rows, width), jnp.float32), dma((fields,))],
        )(*(pltpu.with_memory_space_constraint(x, pltpu.VMEM) for x in near))
        return flux_out.reshape(fields, rows, width), total

    placed = (
        P(("member", "lat"), "lon", None, None),
        P(("member", "lat"), "lon", None),
        P(("member", "lat"), "lon", None),
        P(("member", "lat"), "lon", None),
        P(("member", "lat"), "lon"),
        P(("member", "lat"), "lon"),
        P(("member", "lat"), "lon"),
        P(),
    )
    return jax.shard_map(
        body,
        mesh=mesh,
        in_specs=placed,
        out_specs=(P(None, ("member", "lat"), "lon"), P("member")),
        check_vma=False,
    )
```

```python
import functools

import jax
import jax.numpy as jnp
from jax import lax
from jax.experimental import pallas as pl
from jax.experimental.pallas import tpu as pltpu
from jax.sharding import PartitionSpec as P

MESH = pl.DeviceIdType.MESH
quantum = 1024.0
limb_bits = 16
limb_base = 65536.0
lanes = 128


def carry(upper, lower):
    over = jnp.floor(lower * (1.0 / limb_base))
    return upper + over, lower - over * limb_base


def row_limbs(units):
    upper = jnp.sum((units >> limb_bits).astype(jnp.float32), axis=1, keepdims=True)
    lower = jnp.sum((units & 0xFFFF).astype(jnp.float32), axis=1, keepdims=True)
    return carry(upper, lower)


def join(upper, lower):
    return (upper * limb_base + lower) / quantum


def plan(count):
    middle = (count - 1) / 2
    sends = []
    for me in range(count):
        near = sorted(
            (p for p in range(count) if p != me),
            key=lambda p: (abs(p - me), -((p - me) * (middle - me) > 0)),
        )
        sends.append(near[-1:] + near[:-1])
    late = [row[-1] for row in sends]
    if count ** count >= 2 ** 31 or sorted(late) != list(range(count)):
        return None
    sources = []
    for me in range(count):
        last = late.index(me)
        early = sorted(
            (p for p in range(count) if p not in (me, last)), key=lambda p: abs(p - me)
        )
        sources.append(early + [last])
    return sends, sources


def kernel(
    n_lat, n_lon, cap,
    flux_hbm, frac_hbm, mask_hbm, area_hbm, route_hbm, sea_hbm, wet_hbm, exp_hbm,
    ordered, wetf, coefs, total_ref,
    flux, frac, mask, area, sea, wet, inverse, outgoing, received, routes, exps, sums, cover_in,
    in_sem, route_send, route_recv, bulk_send, bulk_recv, sum_send, sum_recv, cover_sem,
):
    blocks, fields, cells = flux.shape
    rows, width = sea.shape
    band = cells // width
    bits = blocks.bit_length()
    digit = (1 << bits) - 1
    full = cap * n_lon == blocks
    group = n_lat * n_lon
    my_lat = lax.axis_index("lat")
    me = lax.axis_index("lon")

    def peer(offset):
        return {
            "lat": lax.rem(my_lat + offset // n_lon, n_lat),
            "lon": lax.rem(me + offset % n_lon, n_lon),
        }

    loads = [
        pltpu.make_async_copy(src, dst, in_sem.at[i])
        for i, (src, dst) in enumerate((
            (route_hbm, routes.at[pl.ds(0, 1)]), (area_hbm, area), (frac_hbm, frac),
            (mask_hbm, mask), (flux_hbm, flux), (sea_hbm, sea), (wet_hbm, wet), (exp_hbm, exps),
        ))
    ]
    for load in loads:
        load.start()

    barrier = pltpu.get_barrier_semaphore()
    for offset in range(1, group):
        pl.semaphore_signal(barrier, inc=1, device_id=peer(offset), device_id_type=MESH)

    loads[0].wait()

    def digits_of(slot, low, value):
        packed = jnp.int32(0)
        for s in range(blocks):
            r = routes[slot, s]
            hit = (r >= low) & (r < low + blocks)
            packed = jnp.where(hit, (packed << bits) + (value(s, r - low) + 1), packed)
        return [(packed >> (bits * (cap - 1 - c))) & digit for c in range(cap)]

    planned = plan(n_lon)
    if planned:
        place = 1
        for i in range(n_lon - 1):
            place = place * (1 + (n_lon - 1) * ((me + n_lon - 1 - i) // n_lon))
        steps, sources = (
            [
                sum(row[step] * n_lon ** i for i, row in enumerate(table)) // place % n_lon
                for step in range(n_lon - 1)
            ]
            for table in planned
        )
    else:
        steps = [lax.rem(me + d, n_lon) for d in range(1, n_lon)]
        sources = [lax.rem(me + n_lon - d, n_lon) for d in range(1, n_lon)]
    away = [lax.rem(target - me + n_lon, n_lon) for target in steps]
    behind = [lax.rem(me - source + n_lon, n_lon) for source in sources]

    def lon_copy(src, dst, send, recv, target):
        return pltpu.make_async_remote_copy(
            src_ref=src, dst_ref=dst, send_sem=send, recv_sem=recv,
            device_id={"lat": my_lat, "lon": target}, device_id_type=MESH,
        )

    def route_copy(d, src, target):
        return lon_copy(
            routes.at[pl.ds(src, 1)], routes.at[pl.ds(d, 1)],
            route_send.at[d - 1], route_recv.at[d - 1], target,
        )

    def bulk_copy(d, src, first, target):
        return lon_copy(
            src.at[pl.ds(first, cap)], received.at[pl.ds(d * cap, cap)],
            bulk_send.at[d - 1], bulk_recv.at[d - 1], target,
        )

    def fill(target, dst, first):
        picks = digits_of(0, target * blocks, lambda s, row: s)
        for c, pick in enumerate(picks):
            s = jnp.maximum(pick - 1, 0)
            here = pl.ds(s, 1)
            amount = area[here, :] * frac[here, :] * mask[here, :].astype(jnp.float32)
            dst[first + c] = flux[s] * amount

    for load in loads[1:5]:
        load.wait()
    for step, target in enumerate(steps):
        fill(target, outgoing, step * cap)
    last_rows = digits_of(0, steps[-1] * blocks, lambda s, row: row)
    for load in loads[5:]:
        load.wait()

    pl.semaphore_wait(barrier, group - 1)
    cover_copy = lon_copy(wet, cover_in, cover_sem.at[0], cover_sem.at[1], sources[-1])
    route_copies = [route_copy(d, 0, target) for d, target in zip(away, steps)]
    bulk = [
        bulk_copy(d, outgoing, step * cap, target)
        for step, (d, target) in enumerate(zip(away, steps))
    ]
    for copy in route_copies + [cover_copy] + bulk:
        copy.start()
    fill(me, received, 0)
    wetf[...] = wet[...].astype(jnp.float32)
    low = me * blocks

    source_units = jnp.zeros((fields, width), jnp.int32)
    for s in range(blocks):
        here = pl.ds(s, 1)
        amount = area[here, :] * frac[here, :] * mask[here, :].astype(jnp.float32)
        units = (flux[s] * amount * quantum).astype(jnp.int32)
        for r in range(band):
            source_units += units[:, r * width : (r + 1) * width]

    inverse[...] = wetf[...] / sea[...]
    area_units = jnp.zeros((8, width), jnp.int32)
    for i in range(rows // 8):
        part = pl.ds(i * 8, 8)
        area_units += (sea[part, :] * wetf[part, :] * quantum).astype(jnp.int32)

    sub = lax.broadcasted_iota(jnp.int32, (8, lanes), 0)
    lane = lax.broadcasted_iota(jnp.int32, (8, lanes), 1)

    def placed(values, first):
        return sum(
            jnp.where(lane == sub + (first + i) * 8, v, 0.0) for i, v in enumerate(values)
        )

    early = placed(row_limbs(source_units) + row_limbs(area_units), 0)
    power = jnp.zeros((8, lanes), jnp.int32)
    power_row = jnp.zeros((1, lanes), jnp.int32)
    for f in range(fields):
        power = jnp.where(sub == f, exps[f], power)
        power_row = jnp.where(lane[:1] == f, exps[f], power_row)
    scaling = jnp.left_shift(jnp.ones_like(power), power).astype(jnp.float32)
    scaling_row = jnp.left_shift(jnp.ones_like(power_row), power_row).astype(jnp.float32)

    slot_of = [jnp.int32(0)] * blocks

    def settle(d, digits):
        for c in range(cap):
            for n in range(blocks):
                slot_of[n] = jnp.where(digits[c] == n + 1, d * cap + c, slot_of[n])

    target_units = jnp.zeros((fields, width), jnp.int32)
    for d, source in [(0, me)] + list(zip(behind, sources))[:-1]:
        if source is not me:
            route_copy(d, d, source).wait_recv()
        digits = digits_of(d, low, lambda s, row: row)
        settle(d, digits)
        if source is not me:
            bulk_copy(d, received, d * cap, source).wait_recv()
        for c in range(cap):
            row = jnp.maximum(digits[c] - 1, 0)
            for r in range(band):
                cover = wetf[pl.ds(row * band + r, 1), :]
                value = received[d * cap + c, :, r * width : (r + 1) * width]
                units = (cover * value * quantum).astype(jnp.int32)
                if not full:
                    units = units * jnp.minimum(digits[c], 1)
                target_units += units

    cover_copy.wait_recv()
    for c, pick in enumerate(last_rows):
        row = jnp.maximum(pick - 1, 0)
        for r in range(band):
            cover = cover_in[pl.ds(row * band + r, 1), :].astype(jnp.float32)
            value = outgoing[(n_lon - 2) * cap + c, :, r * width : (r + 1) * width]
            units = (cover * value * quantum).astype(jnp.int32)
            if not full:
                units = units * jnp.minimum(pick, 1)
            target_units += units

    mine = jnp.sum(early + placed(row_limbs(target_units), 4), axis=0, keepdims=True)
    sums[pl.ds(0, 1), :] = mine
    sum_copies = []
    for offset in range(1, group):
        copy = pltpu.make_async_remote_copy(
            src_ref=sums.at[pl.ds(0, 1)], dst_ref=sums.at[pl.ds(offset, 1)],
            send_sem=sum_send.at[offset - 1], recv_sem=sum_recv.at[offset - 1],
            device_id=peer(offset), device_id_type=MESH,
        )
        copy.start()
        sum_copies.append(copy)
    d, source = behind[-1], sources[-1]
    route_copy(d, d, source).wait_recv()
    settle(d, digits_of(d, low, lambda s, row: row))
    bulk_copy(d, received, d * cap, source).wait_recv()
    for n in range(blocks):
        slot = slot_of[n]
        for r in range(band):
            line = n * band + r
            value = received[slot, :, r * width : (r + 1) * width]
            ordered[pl.ds(line, fields, stride=rows), :] = value * inverse[line : line + 1, :]

    for copy in sum_copies:
        copy.wait_recv()

    whole = jnp.sum(sums[...], axis=0, keepdims=True)

    def taken(i):
        return jnp.sum(jnp.where(lane == sub + i * 8, whole, 0.0), axis=1, keepdims=True)

    source = join(taken(0), taken(1))
    wet_upper, wet_lower = carry(taken(2), taken(3))
    wet_area = join(
        jnp.sum(wet_upper, axis=0, keepdims=True), jnp.sum(wet_lower, axis=0, keepdims=True)
    )
    target = join(taken(4), taken(5))
    coefs[0] = scaling
    coefs[1] = scaling * ((source - target) / wet_area)

    aligned = pltpu.roll(whole, lanes - 8, 1)
    total_ref[...] = join(whole, aligned) * scaling_row

    for copy in sum_copies + route_copies + bulk + [cover_copy]:
        copy.wait_send()


def finish(ordered, wetf, coefs, total_row, out_hbm, total_ref, out, sems):
    fields = total_ref.shape[0]
    rows = wetf.shape[0]
    copies = []
    for f in range(fields):
        here = pl.ds(f * rows, rows)
        out[here, :] = ordered[here, :] * coefs[0, f : f + 1, :] + wetf[...] * coefs[1, f : f + 1, :]
        copies.append(pltpu.make_async_copy(out.at[here], out_hbm.at[here], sems.at[f]))
        copies[-1].start()
    total_ref[...] = total_row[0, :fields]
    for copy in copies:
        copy.wait()


def solution(mesh):
    n_lat, n_lon = mesh.shape["lat"], mesh.shape["lon"]

    def body(ice_flux, ice_frac, ice_mask, ice_area, route, ocean_area, ocean_wet, exponent):
        blocks, fields, cells = ice_flux.shape[1:]
        rows, width = ocean_area.shape
        cap = max(2, blocks // n_lon)
        group = n_lat * n_lon
        anywhere = pl.BlockSpec(memory_space=pl.ANY)
        vmem = pl.BlockSpec(memory_space=pltpu.VMEM)
        dma = pltpu.SemaphoreType.DMA
        near = pl.pallas_call(
            functools.partial(kernel, n_lat, n_lon, cap),
            out_shape=(
                pltpu.VMEM((fields * rows, width), jnp.float32),
                pltpu.VMEM((rows, width), jnp.float32),
                pltpu.VMEM((2, fields, lanes), jnp.float32),
                pltpu.VMEM((1, lanes), jnp.float32),
            ),
            in_specs=[anywhere] * 8,
            out_specs=(vmem,) * 4,
            scratch_shapes=[
                pltpu.VMEM((blocks, fields, cells), jnp.float32),
                pltpu.VMEM((blocks, cells), jnp.float32),
                pltpu.VMEM((blocks, cells), jnp.int32),
                pltpu.VMEM((blocks, cells), jnp.float32),
                pltpu.VMEM((rows, width), jnp.float32),
                pltpu.VMEM((rows, width), jnp.int32),
                pltpu.VMEM((rows, width), jnp.float32),
                pltpu.VMEM(((n_lon - 1) * cap, fields, cells), jnp.float32),
                pltpu.VMEM((n_lon * cap, fields, cells), jnp.float32),
                pltpu.SMEM((n_lon, blocks), jnp.int32),
                pltpu.SMEM((fields,), jnp.int32),
                pltpu.VMEM((group, lanes), jnp.float32),
                pltpu.VMEM((rows, width), jnp.int32),
                dma((8,)),
                dma((n_lon - 1,)), dma((n_lon - 1,)),
                dma((n_lon - 1,)), dma((n_lon - 1,)),
                dma((group - 1,)), dma((group - 1,)), dma((2,)),
            ],
            compiler_params=pltpu.CompilerParams(collective_id=0, has_side_effects=True),
        )(
            ice_flux[0], ice_frac[0], ice_mask[0], ice_area[0],
            route, ocean_area, ocean_wet, exponent,
        )
        flux_out, total = pl.pallas_call(
            finish,
            out_shape=(
                jax.ShapeDtypeStruct((fields * rows, width), jnp.float32),
                jax.ShapeDtypeStruct((fields,), jnp.float32),
            ),
            in_specs=[vmem] * 4,
            out_specs=(anywhere, vmem),
            scratch_shapes=[pltpu.VMEM((fields * rows, width), jnp.float32), dma((fields,))],
        )(*(pltpu.with_memory_space_constraint(x, pltpu.VMEM) for x in near))
        return flux_out.reshape(fields, rows, width), total

    placed = (
        P(("member", "lat"), "lon", None, None),
        P(("member", "lat"), "lon", None),
        P(("member", "lat"), "lon", None),
        P(("member", "lat"), "lon", None),
        P(("member", "lat"), "lon"),
        P(("member", "lat"), "lon"),
        P(("member", "lat"), "lon"),
        P(),
    )
    return jax.shard_map(
        body,
        mesh=mesh,
        in_specs=placed,
        out_specs=(P(None, ("member", "lat"), "lon"), P("member")),
        check_vma=False,
    )
```
